32 devices in a mesh: row: 2 (over y), col: 4 (over z), layer: 4 (over x, core).
Axes of the slice: x: 2, y: 2, z: 4, core: 2. Of those that a mesh axis runs over, the one named last changes fastest.
Arguments:
- density_tiles: bfloat16 [192, 4, 2, 128, 128], P(('row', 'col')), may hold values from -1.5 to 1.5
- tile_columns: int32 [192, 4, 2], P(('row', 'col')), may hold values from -1 to 191, as said below
Outputs:
- square_tiles: bfloat16 [192, 4, 2, 128, 128], P(('row', 'col'), None, None, 'layer')
The draws below stay inside these ranges and needn't reach their ends.
Inputs may be any that keep to these rules, and one draw needn't show every extreme that they name: `tile_columns`: entry [i, g, s] is a tile column in group g (columns g * 48 to (g + 1) * 48 - 1) or -1; within one block row and group the listed columns are distinct and empty slots come after the listed ones; block row i lists its own column i in the first slot of its group, whose 2 slots are all listed; other groups hold 0 to 2 listed tiles.
All inputs are finite; a program needn't handle non-finite values.
Results may differ from the reference program's by a relative error of at most 0.0048.
Values may be sent and summed in bfloat16 or wider, within the bound.
A program may use at most 128 MiB of HBM per device.

```python
import jax
import jax.numpy as jnp
from jax import lax

TB = 128
NB = 192
KG = 2
NGROUP = 4
GWIDTH = 48
N_LAYER = 4


def draw_tile_columns(key, part):
    shuffle_key, anchor_key, count_key = jax.random.split(jax.random.fold_in(key, 17), 3)
    row_index = jnp.arange(NB, dtype=jnp.int32)
    group_index = jnp.arange(NGROUP, dtype=jnp.int32)

    def shuffled(sub_key):
        return jax.random.permutation(sub_key, GWIDTH - 1)[:KG - 1].astype(jnp.int32)
    offsets = jax.vmap(shuffled)(jax.random.split(shuffle_key, NB * NGROUP)).reshape(NB, NGROUP, KG - 1)
    anchors = jax.random.randint(anchor_key, (NB, NGROUP), 0, GWIDTH).astype(jnp.int32)
    own_group = row_index // GWIDTH
    is_own = own_group[:, None] == group_index[None, :]
    anchors = jnp.where(is_own, (row_index % GWIDTH)[:, None], anchors)
    local_column = jnp.concatenate([anchors[:, :, None], (anchors[:, :, None] + 1 + offsets) % GWIDTH], axis=-1)
    apart = jnp.abs(group_index[None, :] - own_group[:, None])
    distance = jnp.minimum(apart, NGROUP - apart)
    drawn_count = jax.random.randint(count_key, (NB, NGROUP), 0, KG + 1).astype(jnp.int32)
    live_count = jnp.where(distance <= 1, KG, drawn_count)
    slot_index = jnp.arange(KG, dtype=jnp.int32)
    columns = local_column + group_index[None, :, None] * GWIDTH
    return jnp.where(slot_index[None, None, :] < live_count[:, :, None], columns, -1).astype(jnp.int32)


def block_scale(own_key, dims, shards, smallest, high):
    factor_of = 1.0
    for axis_at, parts in shards:
        steps = jax.random.uniform(jax.random.fold_in(jax.random.fold_in(own_key, 6), axis_at), (parts,), jnp.float32, smallest / len(shards), high / len(shards))
        factor_of = factor_of * jnp.repeat(jnp.exp(steps), dims[axis_at] // parts).reshape((-1,) + (1,) * (len(dims) - 1 - axis_at))
    return factor_of


def gaussian(key, extent, width, most, cuts=(), kind=jnp.bfloat16):
    gain = block_scale(key, extent, cuts, -0.22, 0.18) if cuts else 1.0
    result = jax.random.normal(key, extent, jnp.float32) * width * gain
    return jnp.minimum(jnp.maximum(result, -most), most).astype(kind)


def setup_inputs(seed: int = 0) -> dict:
    key_list = jax.random.split(jax.random.key(seed), 3)
    density_tiles = gaussian(key_list[0], (NB, NGROUP, KG, TB, TB), 0.25, 1.5, ((0, 8),))
    tile_columns = draw_tile_columns(jax.random.fold_in(key_list[2], 71), 0)
    return dict(density_tiles=density_tiles, tile_columns=tile_columns)


def reference(density_tiles, tile_columns):
    block_count, group_count, group_slots, tile_side, _ = density_tiles.shape
    row_width = group_count * group_slots
    per_layer = group_count // N_LAYER
    flat_tiles = density_tiles.reshape(block_count, row_width, tile_side, tile_side)
    flat_columns = tile_columns.reshape(block_count, row_width)

    def one_row(row_index):
        own_columns = flat_columns[row_index]
        own_tiles = flat_tiles[row_index]
        is_live = own_columns >= 0
        inner_rows = jnp.where(is_live, own_columns, 0).astype(jnp.int32)
        inner_columns = flat_columns[inner_rows]
        matches = (inner_columns[:, None, :] == own_columns[None, :, None]) & is_live[:, None, None] & is_live[None, :, None]
        slot_index = jnp.argmax(matches.astype(jnp.int32), axis=-1).astype(jnp.int32)
        located = jnp.any(matches, axis=-1)
        selected = flat_tiles[inner_rows[:, None], slot_index].astype(jnp.float32)
        selected = jnp.where(located[:, :, None, None], selected, jnp.float32(0.0))
        left_tiles = own_tiles.astype(jnp.float32).reshape(N_LAYER, per_layer * group_slots, tile_side, tile_side)
        selected = selected.reshape(N_LAYER, per_layer * group_slots, row_width, tile_side, tile_side)
        partial_value = jnp.einsum("larc,lascd->lsrd", left_tiles, selected)
        rounded = lax.optimization_barrier(partial_value.astype(jnp.bfloat16))
        layer_total = jnp.sum(rounded.astype(jnp.float32), axis=0)
        return layer_total.astype(jnp.bfloat16).reshape(group_count, group_slots, tile_side, tile_side)

    return lax.map(one_row, jnp.arange(block_count, dtype=jnp.int32))
```

```python
import functools

import jax
import jax.numpy as jnp
from jax import lax
from jax.experimental import pallas as pl
from jax.experimental.pallas import tpu as pltpu
from jax.sharding import PartitionSpec as P

MESH = pl.DeviceIdType.MESH


def divisor(total, most):
    return max(d for d in range(1, most + 1) if total % d == 0)


def kernel(
    sizes, columns_ref, tiles_ref, meta_ref, out_ref,
    left, right, meta_all, meta_smem, stage,
    local_sem, meta_send, meta_recv, send_sem, recv_sem, out_send, out_recv,
):
    row_count, col_count, layer_count, chunks, out_chunks, is_balanced = sizes
    n, group_count, slots, tile, _ = tiles_ref.shape
    cells = row_count * col_count
    per_layer = group_count // layer_count
    quarter = tile // layer_count
    width = group_count * slots
    r, c, l = lax.axis_index("row"), lax.axis_index("col"), lax.axis_index("layer")
    me = r * col_count + c
    own_groups = pl.ds(l * per_layer, per_layer)

    own_copy = pltpu.make_async_copy(
        tiles_ref.at[:, own_groups], right.at[pl.ds(me * n, n)], local_sem.at[0]
    )
    left_copy = pltpu.make_async_copy(tiles_ref, left, local_sem.at[1])
    meta_copy = pltpu.make_async_copy(meta_ref, meta_all.at[pl.ds(me * n, n)], local_sem.at[2])
    own_copy.start()
    meta_copy.start()
    left_copy.start()
    right[cells * n] = jnp.zeros(right.shape[1:], right.dtype)

    def cell_id(offset):
        target = lax.rem(me + offset, cells)
        return {"row": lax.div(target, col_count), "col": lax.rem(target, col_count)}

    def layer_id(offset):
        return {"layer": lax.rem(l + offset, layer_count)}

    barrier = pltpu.get_barrier_semaphore()
    for offset in range(1, cells):
        pl.semaphore_signal(barrier, inc=1, device_id=cell_id(offset), device_id_type=MESH)
    for offset in range(1, layer_count):
        pl.semaphore_signal(barrier, inc=1, device_id=layer_id(offset), device_id_type=MESH)
    pl.semaphore_wait(barrier, cells - 1 + layer_count - 1)
    own_copy.wait()

    step_rows = n // chunks
    sent = []

    def rows_of(cell, chunk):
        return pl.ds(cell * n + chunk * step_rows, step_rows)

    def copy_of(cell, chunk, way, device):
        return pltpu.make_async_remote_copy(
            src_ref=right.at[rows_of(cell, chunk)],
            dst_ref=right.at[rows_of(cell, chunk)],
            send_sem=send_sem.at[way, cell, chunk],
            recv_sem=recv_sem.at[cell, chunk],
            device_id=device,
            device_id_type=MESH,
        )

    ways = {
        "up": (0, c < col_count - 1, {"col": jnp.minimum(c + 1, col_count - 1)}),
        "down": (1, c > 0, {"col": jnp.maximum(c - 1, 0)}),
        "south": (2, r < row_count - 1, {"row": jnp.minimum(r + 1, row_count - 1)}),
        "north": (3, r > 0, {"row": jnp.maximum(r - 1, 0)}),
    }

    def send(cell, chunk, way, condition=True):
        index, exists, device = ways[way]
        wanted = jnp.logical_and(exists, condition)

        @pl.when(wanted)
        def _():
            copy_of(cell, chunk, index, device).start()

        sent.append((wanted, cell, chunk, index, device))

    def await_arrival(cell, chunk):
        copy_of(cell, chunk, 0, {"col": c}).wait_recv()

    for chunk in range(chunks):
        for way in ("up", "down", "south", "north"):
            send(me, chunk, way)

    meta_copy.wait()
    meta_copies = []
    for offset in range(1, cells):
        copy = pltpu.make_async_remote_copy(
            src_ref=meta_ref,
            dst_ref=meta_all.at[pl.ds(me * n, n)],
            send_sem=meta_send.at[offset],
            recv_sem=meta_recv.at[offset],
            device_id=cell_id(offset),
            device_id_type=MESH,
        )
        copy.start()
        meta_copies.append(copy)

    even = lax.rem(c, 2) == 0
    for step in range(1, col_count):
        for chunk in range(chunks):
            for origin, has, way, is_pair in (
                (c - step, c >= step, "up", jnp.logical_not(even)),
                (c + step, c + step < col_count, "down", even),
            ):
                origin = jnp.clip(origin, 0, col_count - 1)
                cell = r * col_count + origin

                @pl.when(has)
                def _():
                    await_arrival(cell, chunk)

                send(cell, chunk, way, has)
                across = has
                if is_balanced and step == 1 and chunk >= chunks // 2:
                    across = jnp.logical_and(has, jnp.logical_not(is_pair))
                send(cell, chunk, "south", across)
                send(cell, chunk, "north", across)

    if is_balanced:
        other = (1 - r) * col_count + c
        for chunk in range(chunks):
            await_arrival(other, chunk)
            if chunk >= chunks // 2:
                send(other, chunk, "up", even)
                send(other, chunk, "down", jnp.logical_not(even))
        for step in range(1, col_count):
            origin = (1 - r) * col_count + lax.rem(c + step, col_count)
            for chunk in range(chunks):
                await_arrival(origin, chunk)
    else:
        for step in range(1, row_count):
            for shift in range(col_count):
                for chunk in range(chunks):
                    for origin, has, way in (
                        (r - step, r >= step, "south"),
                        (r + step, r + step < row_count, "north"),
                    ):
                        origin = jnp.clip(origin, 0, row_count - 1)
                        cell = origin * col_count + lax.rem(c + shift, col_count)

                        @pl.when(has)
                        def _():
                            await_arrival(cell, chunk)

                        send(cell, chunk, way, has)

    for copy in meta_copies:
        copy.wait()
    table_copy = pltpu.make_async_copy(meta_all, meta_smem, local_sem.at[3])
    table_copy.start()
    table_copy.wait()
    left_copy.wait()

    def one_row(i, carry):
        targets = [
            columns_ref[i * width + l * per_layer * slots + s] for s in range(per_layer * slots)
        ]
        strips = []
        for a in range(width):
            k = columns_ref[i * width + a]
            inner = jnp.maximum(k, 0)
            pieces = []
            for s in range(per_layer * slots):
                group = s // slots
                row_index = jnp.int32(cells * n)
                slot_index = jnp.int32(0)
                is_live = (k >= 0) & (targets[s] >= 0)
                for t in range(slots):
                    hit = (meta_smem[inner, 0, group * slots + t] == targets[s]) & is_live
                    row_index = jnp.where(hit, inner, row_index)
                    slot_index = jnp.where(hit, t, slot_index)
                pieces.append(right[row_index, group, slot_index])
            strips.append(jnp.concatenate(pieces, axis=1))
        rights = jnp.concatenate(strips, axis=0)
        lefts = jnp.concatenate(
            [left[i, a // slots, a % slots] for a in range(width)], axis=1
        )
        total = jnp.dot(lefts, rights, preferred_element_type=jnp.float32).astype(stage.dtype)
        for q in range(layer_count):
            for s in range(per_layer * slots):
                stage[q, i, s // slots, s % slots] = total[
                    q * quarter:(q + 1) * quarter, s * tile:(s + 1) * tile
                ]
        return carry

    out_rows = n // out_chunks

    def out_copies(chunk):
        rows = pl.ds(chunk * out_rows, out_rows)
        copies = []
        for offset in range(layer_count):
            q = lax.rem(l + offset, layer_count)
            if offset == 0:
                copies.append(pltpu.make_async_copy(
                    stage.at[q, rows], out_ref.at[rows, own_groups], out_send.at[0, chunk]
                ))
            else:
                copies.append(pltpu.make_async_remote_copy(
                    src_ref=stage.at[q, rows],
                    dst_ref=out_ref.at[rows, own_groups],
                    send_sem=out_send.at[offset, chunk],
                    recv_sem=out_recv.at[offset, chunk],
                    device_id=layer_id(offset),
                    device_id_type=MESH,
                ))
        return copies

    all_out = []
    for chunk in range(out_chunks + 1):
        if chunk < out_chunks:
            lax.fori_loop(chunk * out_rows, (chunk + 1) * out_rows, one_row, 0)
        if chunk > 0:
            copies = out_copies(chunk - 1)
            for copy in copies[1:] + copies[:1]:
                copy.start()
            all_out.extend(copies)

    for wanted, cell, chunk, index, device in sent:
        @pl.when(wanted)
        def _():
            copy_of(cell, chunk, index, device).wait_send()

    for copy in all_out:
        copy.wait()


def on_device(density_tiles, tile_columns):
    row_count = lax.axis_size("row")
    col_count = lax.axis_size("col")
    layer_count = lax.axis_size("layer")
    n, group_count, slots, tile, _ = density_tiles.shape
    cells = row_count * col_count
    per_layer = group_count // layer_count
    quarter = tile // layer_count
    kept = per_layer * slots
    chunks = divisor(n, 4)
    out_chunks = divisor(n, 4)
    is_balanced = row_count == 2 and col_count % 2 == 0 and chunks % 2 == 0
    own = lax.dynamic_slice_in_dim(tile_columns, lax.axis_index("layer") * per_layer, per_layer, 1)
    meta = jnp.pad(own.reshape(n, 1, kept), ((0, 0), (0, 0), (0, 128 - kept)), constant_values=-1)
    dtype = density_tiles.dtype
    sizes = (row_count, col_count, layer_count, chunks, out_chunks, is_balanced)
    return pl.pallas_call(
        functools.partial(kernel, sizes),
        out_shape=jax.ShapeDtypeStruct((n, group_count, slots, quarter, tile), dtype),
        in_specs=[
            pl.BlockSpec(memory_space=pltpu.SMEM),
            pl.BlockSpec(memory_space=pl.ANY),
            pl.BlockSpec(memory_space=pltpu.VMEM),
        ],
        out_specs=pl.BlockSpec(memory_space=pl.ANY),
        scratch_shapes=[
            pltpu.VMEM(density_tiles.shape, dtype),
            pltpu.VMEM((cells * n + 1, per_layer, slots, tile, tile), dtype),
            pltpu.VMEM((cells * n, 1, 128), jnp.int32),
            pltpu.SMEM((cells * n, 1, 128), jnp.int32),
            pltpu.VMEM((layer_count, n, per_layer, slots, quarter, tile), dtype),
            pltpu.SemaphoreType.DMA((4,)),
            pltpu.SemaphoreType.DMA((cells,)),
            pltpu.SemaphoreType.DMA((cells,)),
            pltpu.SemaphoreType.DMA((4, cells, chunks)),
            pltpu.SemaphoreType.DMA((cells, chunks)),
            pltpu.SemaphoreType.DMA((layer_count, out_chunks)),
            pltpu.SemaphoreType.DMA((layer_count, out_chunks)),
        ],
        compiler_params=pltpu.CompilerParams(
            collective_id=0, has_side_effects=True, vmem_limit_bytes=60 * 1024 * 1024
        ),
    )(tile_columns.reshape(-1), density_tiles, meta)


def solution(mesh):
    in_specs = (P(("row", "col"), None, None, None, None), P(("row", "col"), None, None))
    out_specs = P(("row", "col"), None, None, "layer", None)
    return jax.shard_map(
        on_device, mesh=mesh, in_specs=in_specs, out_specs=out_specs, check_vma=False
    )
```

```python
import functools

import jax
import jax.numpy as jnp
from jax import lax
from jax.experimental import pallas as pl
from jax.experimental.pallas import tpu as pltpu
from jax.sharding import PartitionSpec as P

MESH = pl.DeviceIdType.MESH


def divisor(total, most):
    return max(d for d in range(1, most + 1) if total % d == 0)


def kernel(
    sizes, columns_ref, tiles_ref, meta_ref, out_ref,
    left, right, meta_all, meta_smem, stage,
    local_sem, meta_send, meta_recv, send_sem, recv_sem, out_send, out_recv,
):
    row_count, col_count, layer_count, chunks, out_chunks, is_balanced = sizes
    n, group_count, slots, tile, _ = tiles_ref.shape
    cells = row_count * col_count
    per_layer = group_count // layer_count
    quarter = tile // layer_count
    width = group_count * slots
    r, c, l = lax.axis_index("row"), lax.axis_index("col"), lax.axis_index("layer")
    me = r * col_count + c
    own_groups = pl.ds(l * per_layer, per_layer)

    own_copy = pltpu.make_async_copy(
        tiles_ref.at[:, own_groups], right.at[pl.ds(me * n, n)], local_sem.at[0]
    )
    left_copy = pltpu.make_async_copy(tiles_ref, left, local_sem.at[1])
    meta_copy = pltpu.make_async_copy(meta_ref, meta_all.at[pl.ds(me * n, n)], local_sem.at[2])
    own_copy.start()
    meta_copy.start()
    left_copy.start()
    right[cells * n] = jnp.zeros(right.shape[1:], right.dtype)

    def cell_id(offset):
        target = lax.rem(me + offset, cells)
        return {"row": lax.div(target, col_count), "col": lax.rem(target, col_count)}

    def layer_id(offset):
        return {"layer": lax.rem(l + offset, layer_count)}

    barrier = pltpu.get_barrier_semaphore()
    for offset in range(1, cells):
        pl.semaphore_signal(barrier, inc=1, device_id=cell_id(offset), device_id_type=MESH)
    for offset in range(1, layer_count):
        pl.semaphore_signal(barrier, inc=1, device_id=layer_id(offset), device_id_type=MESH)
    pl.semaphore_wait(barrier, cells - 1 + layer_count - 1)
    own_copy.wait()

    step_rows = n // chunks
    sent = []

    def rows_of(cell, chunk):
        return pl.ds(cell * n + chunk * step_rows, step_rows)

    def copy_of(cell, chunk, way, device):
        return pltpu.make_async_remote_copy(
            src_ref=right.at[rows_of(cell, chunk)],
            dst_ref=right.at[rows_of(cell, chunk)],
            send_sem=send_sem.at[way, cell, chunk],
            recv_sem=recv_sem.at[cell, chunk],
            device_id=device,
            device_id_type=MESH,
        )

    ways = {
        "up": (0, c < col_count - 1, {"col": jnp.minimum(c + 1, col_count - 1)}),
        "down": (1, c > 0, {"col": jnp.maximum(c - 1, 0)}),
        "south": (2, r < row_count - 1, {"row": jnp.minimum(r + 1, row_count - 1)}),
        "north": (3, r > 0, {"row": jnp.maximum(r - 1, 0)}),
    }

    def send(cell, chunk, way, condition=True):
        index, exists, device = ways[way]
        wanted = jnp.logical_and(exists, condition)

        @pl.when(wanted)
        def _():
            copy_of(cell, chunk, index, device).start()

        sent.append((wanted, cell, chunk, index, device))

    def await_arrival(cell, chunk):
        copy_of(cell, chunk, 0, {"col": c}).wait_recv()

    for chunk in range(chunks):
        for way in ("up", "down", "south", "north"):
            send(me, chunk, way)

    meta_copy.wait()
    meta_copies = []
    for offset in range(1, cells):
        copy = pltpu.make_async_remote_copy(
            src_ref=meta_ref,
            dst_ref=meta_all.at[pl.ds(me * n, n)],
            send_sem=meta_send.at[offset],
            recv_sem=meta_recv.at[offset],
            device_id=cell_id(offset),
            device_id_type=MESH,
        )
        copy.start()
        meta_copies.append(copy)

    even = lax.rem(c, 2) == 0
    for step in range(1, col_count):
        for chunk in range(chunks):
            for origin, has, way, is_pair in (
                (c - step, c >= step, "up", jnp.logical_not(even)),
                (c + step, c + step < col_count, "down", even),
            ):
                origin = jnp.clip(origin, 0, col_count - 1)
                cell = r * col_count + origin

                @pl.when(has)
                def _():
                    await_arrival(cell, chunk)

                send(cell, chunk, way, has)
                across = has
                if is_balanced and step == 1 and chunk >= chunks // 2:
                    across = jnp.logical_and(has, jnp.logical_not(is_pair))
                send(cell, chunk, "south", across)
                send(cell, chunk, "north", across)

    if is_balanced:
        other = (1 - r) * col_count + c
        for chunk in range(chunks):
            await_arrival(other, chunk)
            if chunk >= chunks // 2:
                send(other, chunk, "up", even)
                send(other, chunk, "down", jnp.logical_not(even))
        for step in range(1, col_count):
            origin = (1 - r) * col_count + lax.rem(c + step, col_count)
            for chunk in range(chunks):
                await_arrival(origin, chunk)
    else:
        for step in range(1, row_count):
            for shift in range(col_count):
                for chunk in range(chunks):
                    for origin, has, way in (
                        (r - step, r >= step, "south"),
                        (r + step, r + step < row_count, "north"),
                    ):
                        origin = jnp.clip(origin, 0, row_count - 1)
                        cell = origin * col_count + lax.rem(c + shift, col_count)

                        @pl.when(has)
                        def _():
                            await_arrival(cell, chunk)

                        send(cell, chunk, way, has)

    for copy in meta_copies:
        copy.wait()
    table_copy = pltpu.make_async_copy(meta_all, meta_smem, local_sem.at[3])
    table_copy.start()
    table_copy.wait()
    left_copy.wait()

    def one_row(i, carry):
        targets = [
            columns_ref[i * width + l * per_layer * slots + s] for s in range(per_layer * slots)
        ]
        strips = []
        for a in range(width):
            k = columns_ref[i * width + a]
            inner = jnp.maximum(k, 0)
            pieces = []
            for s in range(per_layer * slots):
                group = s // slots
                row_index = jnp.int32(cells * n)
                slot_index = jnp.int32(0)
                is_live = (k >= 0) & (targets[s] >= 0)
                for t in range(slots):
                    hit = (meta_smem[inner, 0, group * slots + t] == targets[s]) & is_live
                    row_index = jnp.where(hit, inner, row_index)
                    slot_index = jnp.where(hit, t, slot_index)
                pieces.append(right[row_index, group, slot_index])
            strips.append(jnp.concatenate(pieces, axis=1))
        rights = jnp.concatenate(strips, axis=0)
        lefts = jnp.concatenate(
            [left[i, a // slots, a % slots] for a in range(width)], axis=1
        )
        total = jnp.dot(lefts, rights, preferred_element_type=jnp.float32).astype(stage.dtype)
        for q in range(layer_count):
            for s in range(per_layer * slots):
                stage[q, i, s // slots, s % slots] = total[
                    q * quarter:(q + 1) * quarter, s * tile:(s + 1) * tile
                ]
        return carry

    out_rows = n // out_chunks

    def out_copies(chunk):
        rows = pl.ds(chunk * out_rows, out_rows)
        copies = []
        for offset in range(layer_count):
            q = lax.rem(l + offset, layer_count)
            if offset == 0:
                copies.append(pltpu.make_async_copy(
                    stage.at[q, rows], out_ref.at[rows, own_groups], out_send.at[0, chunk]
                ))
            else:
                copies.append(pltpu.make_async_remote_copy(
                    src_ref=stage.at[q, rows],
                    dst_ref=out_ref.at[rows, own_groups],
                    send_sem=out_send.at[offset, chunk],
                    recv_sem=out_recv.at[offset, chunk],
                    device_id=layer_id(offset),
                    device_id_type=MESH,
                ))
        return copies

    all_out = []
    for chunk in range(out_chunks + 1):
        if chunk < out_chunks:
            lax.fori_loop(chunk * out_rows, (chunk + 1) * out_rows, one_row, 0)
        if chunk > 0:
            copies = out_copies(chunk - 1)
            for copy in copies[1:] + copies[:1]:
                copy.start()
            all_out.extend(copies)

    for wanted, cell, chunk, index, device in sent:
        @pl.when(wanted)
        def _():
            copy_of(cell, chunk, index, device).wait_send()

    for copy in all_out:
        copy.wait()


def on_device(density_tiles, tile_columns):
    row_count = lax.axis_size("row")
    col_count = lax.axis_size("col")
    layer_count = lax.axis_size("layer")
    n, group_count, slots, tile, _ = density_tiles.shape
    cells = row_count * col_count
    per_layer = group_count // layer_count
    quarter = tile // layer_count
    kept = per_layer * slots
    chunks = divisor(n, 4)
    out_chunks = divisor(n, 4)
    is_balanced = row_count == 2 and col_count % 2 == 0 and chunks % 2 == 0
    own = lax.dynamic_slice_in_dim(tile_columns, lax.axis_index("layer") * per_layer, per_layer, 1)
    meta = jnp.pad(own.reshape(n, 1, kept), ((0, 0), (0, 0), (0, 128 - kept)), constant_values=-1)
    dtype = density_tiles.dtype
    sizes = (row_count, col_count, layer_count, chunks, out_chunks, is_balanced)
    return pl.pallas_call(
        functools.partial(kernel, sizes),
        out_shape=jax.ShapeDtypeStruct((n, group_count, slots, quarter, tile), dtype),
        in_specs=[
            pl.BlockSpec(memory_space=pltpu.SMEM),
            pl.BlockSpec(memory_space=pl.ANY),
            pl.BlockSpec(memory_space=pltpu.VMEM),
        ],
        out_specs=pl.BlockSpec(memory_space=pl.ANY),
        scratch_shapes=[
            pltpu.VMEM(density_tiles.shape, dtype),
            pltpu.VMEM((cells * n + 1, per_layer, slots, tile, tile), dtype),
            pltpu.VMEM((cells * n, 1, 128), jnp.int32),
            pltpu.SMEM((cells * n, 1, 128), jnp.int32),
            pltpu.VMEM((layer_count, n, per_layer, slots, quarter, tile), dtype),
            pltpu.SemaphoreType.DMA((4,)),
            pltpu.SemaphoreType.DMA((cells,)),
            pltpu.SemaphoreType.DMA((cells,)),
            pltpu.SemaphoreType.DMA((4, cells, chunks)),
            pltpu.SemaphoreType.DMA((cells, chunks)),
            pltpu.SemaphoreType.DMA((layer_count, out_chunks)),
            pltpu.SemaphoreType.DMA((layer_count, out_chunks)),
        ],
        compiler_params=pltpu.CompilerParams(
            collective_id=0, has_side_effects=True, vmem_limit_bytes=60 * 1024 * 1024
        ),
    )(tile_columns.reshape(-1), density_tiles, meta)


def paired_kernel(
    sizes, tiles_ref, meta_ref, out_ref,
    left, right, meta_all, meta_smem, stage,
    local_sem, meta_send, meta_recv, send_sem, recv_sem, left_send, left_recv, out_send, out_recv,
):
    col_count, layer_count, chunks, out_chunks = sizes
    n, group_count, slots, tile, _ = tiles_ref.shape
    cells = 2 * col_count
    per_layer = group_count // layer_count
    quarter = tile // layer_count
    width = group_count * slots
    r, c, l = lax.axis_index("row"), lax.axis_index("col"), lax.axis_index("layer")
    high, k = lax.div(l, 2), lax.rem(l, 2)
    me = r * col_count + c
    base = k * col_count + c
    is_home = k == r
    is_guest = jnp.logical_not(is_home)
    group = 2 * high + r
    own_groups = pl.ds(group * per_layer, per_layer)
    other_groups = pl.ds((2 * high + 1 - r) * per_layer, per_layer)
    facing = {"row": 1 - r}
    partner = {"layer": 2 * high + 1 - k}

    own_copy = pltpu.make_async_copy(
        tiles_ref.at[:, own_groups], right.at[pl.ds(me * n, n)], local_sem.at[0]
    )
    left_copy = pltpu.make_async_copy(tiles_ref, left, local_sem.at[1])
    meta_copy = pltpu.make_async_copy(meta_ref, meta_all.at[pl.ds(me * n, n)], local_sem.at[2])
    own_copy.start()
    meta_copy.start()

    @pl.when(is_home)
    def _():
        left_copy.start()

    right[cells * n] = jnp.zeros(right.shape[1:], right.dtype)

    def cell_id(offset):
        target = lax.rem(me + offset, cells)
        return {"row": lax.div(target, col_count), "col": lax.rem(target, col_count)}

    barrier = pltpu.get_barrier_semaphore()
    for offset in range(1, cells):
        pl.semaphore_signal(barrier, inc=1, device_id=cell_id(offset), device_id_type=MESH)
    for offset in range(1, layer_count):
        for row in (r, 1 - r):
            pl.semaphore_signal(
                barrier,
                inc=1,
                device_id={"row": row, "layer": lax.rem(l + offset, layer_count)},
                device_id_type=MESH,
            )
    pl.semaphore_wait(barrier, cells - 1 + 2 * (layer_count - 1))

    step_rows = n // chunks
    sent = []

    def rows_of(cell, chunk):
        return pl.ds(cell * n + chunk * step_rows, step_rows)

    def copy_of(cell, chunk, way, device):
        source = right.at[rows_of(cell, chunk)]
        if way == 3:
            source = tiles_ref.at[pl.ds(chunk * step_rows, step_rows), other_groups]
        return pltpu.make_async_remote_copy(
            src_ref=source,
            dst_ref=right.at[rows_of(cell, chunk)],
            send_sem=send_sem.at[way, cell, chunk],
            recv_sem=recv_sem.at[cell, chunk],
            device_id=device,
            device_id_type=MESH,
        )

    ways = {
        "up": (0, c < col_count - 1, {"col": jnp.minimum(c + 1, col_count - 1)}),
        "down": (1, c > 0, {"col": jnp.maximum(c - 1, 0)}),
        "partner": (2, True, partner),
        "facing": (3, True, facing),
    }

    def send(cell, chunk, way, condition):
        index, exists, device = ways[way]
        wanted = jnp.logical_and(exists, condition)

        @pl.when(wanted)
        def _():
            copy_of(cell, chunk, index, device).start()

        sent.append((wanted, cell, chunk, index, device))

    def await_arrival(cell, chunk, condition):
        @pl.when(condition)
        def _():
            copy_of(cell, chunk, 2, partner).wait_recv()

    for chunk in range(chunks):
        send(me, chunk, "facing", is_home)
    own_copy.wait()
    for chunk in range(chunks):
        for way in ("up", "down"):
            send(me, chunk, way, is_home)
    left_out = pltpu.make_async_remote_copy(
        src_ref=tiles_ref, dst_ref=left, send_sem=left_send, recv_sem=left_recv,
        device_id=facing, device_id_type=MESH,
    )

    meta_copy.wait()
    meta_copies = []
    for offset in range(1, cells):
        copy = pltpu.make_async_remote_copy(
            src_ref=meta_ref,
            dst_ref=meta_all.at[pl.ds(me * n, n)],
            send_sem=meta_send.at[offset],
            recv_sem=meta_recv.at[offset],
            device_id=cell_id(offset),
            device_id_type=MESH,
        )
        copy.start()
        meta_copies.append(copy)

    @pl.when(is_home)
    def _():
        left_out.start()

    for chunk in range(chunks):
        await_arrival(base, chunk, is_guest)
        for way in ("up", "down", "partner"):
            send(base, chunk, way, is_guest)

    for step in range(1, col_count):
        for chunk in range(chunks):
            for origin, has, way in (
                (c - step, c >= step, "up"),
                (c + step, c + step < col_count, "down"),
            ):
                cell = k * col_count + jnp.clip(origin, 0, col_count - 1)
                await_arrival(cell, chunk, has)
                send(cell, chunk, way, has)
                send(cell, chunk, "partner", has)

    for chunk in range(chunks):
        await_arrival((1 - k) * col_count + c, chunk, is_home)
    for step in range(1, col_count):
        cell = (1 - k) * col_count + lax.rem(c + step, col_count)
        for chunk in range(chunks):
            await_arrival(cell, chunk, True)

    for copy in meta_copies:
        copy.wait()
    table_copy = pltpu.make_async_copy(meta_all, meta_smem, local_sem.at[3])
    table_copy.start()
    table_copy.wait()

    @pl.when(is_home)
    def _():
        left_copy.wait()

    @pl.when(is_guest)
    def _():
        left_out.wait_recv()

    first = group * per_layer * slots

    def one_row(i, carry):
        block_row = base * n + i
        targets = [meta_smem[block_row, 0, first + s] for s in range(per_layer * slots)]
        strips = []
        for a in range(width):
            column = meta_smem[block_row, 0, a]
            inner = jnp.maximum(column, 0)
            pieces = []
            for s in range(per_layer * slots):
                part = s // slots
                row_index = jnp.int32(cells * n)
                slot_index = jnp.int32(0)
                is_live = (column >= 0) & (targets[s] >= 0)
                for t in range(slots):
                    hit = (meta_smem[inner, 0, first + part * slots + t] == targets[s]) & is_live
                    row_index = jnp.where(hit, inner, row_index)
                    slot_index = jnp.where(hit, t, slot_index)
                pieces.append(right[row_index, part, slot_index])
            strips.append(jnp.concatenate(pieces, axis=1))
        rights = jnp.concatenate(strips, axis=0)
        lefts = jnp.concatenate(
            [left[i, a // slots, a % slots] for a in range(width)], axis=1
        )
        total = jnp.dot(lefts, rights, preferred_element_type=jnp.float32).astype(stage.dtype)
        for q in range(layer_count):
            for s in range(per_layer * slots):
                stage[q, i, s // slots, s % slots] = total[
                    q * quarter:(q + 1) * quarter, s * tile:(s + 1) * tile
                ]
        return carry

    out_rows = n // out_chunks

    def out_copy(chunk, q, source):
        rows = pl.ds(chunk * out_rows, out_rows)
        return pltpu.make_async_remote_copy(
            src_ref=stage.at[q, rows],
            dst_ref=out_ref.at[rows, pl.ds(source * per_layer, per_layer)],
            send_sem=out_send.at[q, chunk],
            recv_sem=out_recv.at[source, chunk],
            device_id={"row": k, "layer": q},
            device_id_type=MESH,
        )

    def kept_copy(chunk):
        rows = pl.ds(chunk * out_rows, out_rows)
        return pltpu.make_async_copy(
            stage.at[l, rows], out_ref.at[rows, own_groups], out_send.at[l, chunk]
        )

    for chunk in range(out_chunks + 1):
        if chunk < out_chunks:
            lax.fori_loop(chunk * out_rows, (chunk + 1) * out_rows, one_row, 0)
        if chunk > 0:
            for offset in range(layer_count - 1, -1, -1):
                q = lax.rem(l + offset, layer_count)
                if offset:
                    out_copy(chunk - 1, q, group).start()
                else:
                    @pl.when(is_guest)
                    def _():
                        out_copy(chunk - 1, q, group).start()

                    @pl.when(is_home)
                    def _():
                        kept_copy(chunk - 1).start()

    for wanted, cell, chunk, index, device in sent:
        @pl.when(wanted)
        def _():
            copy_of(cell, chunk, index, device).wait_send()

    @pl.when(is_home)
    def _():
        left_out.wait_send()

    for chunk in range(out_chunks):
        for offset in range(layer_count):
            q = lax.rem(l + offset, layer_count)
            source = lax.rem(group + offset, layer_count)
            if offset:
                out_copy(chunk, q, source).wait()
            else:
                @pl.when(is_guest)
                def _():
                    out_copy(chunk, q, source).wait()

                @pl.when(is_home)
                def _():
                    kept_copy(chunk).wait()


def on_device_paired(density_tiles, tile_columns):
    col_count = lax.axis_size("col")
    layer_count = lax.axis_size("layer")
    n, group_count, slots, tile, _ = density_tiles.shape
    cells = 2 * col_count
    per_layer = group_count // layer_count
    quarter = tile // layer_count
    width = group_count * slots
    chunks = divisor(n, 4)
    out_chunks = divisor(n, 8)
    lanes = -(-width // 128) * 128
    meta = jnp.pad(
        tile_columns.reshape(n, 1, width), ((0, 0), (0, 0), (0, lanes - width)), constant_values=-1
    )
    dtype = density_tiles.dtype
    return pl.pallas_call(
        functools.partial(paired_kernel, (col_count, layer_count, chunks, out_chunks)),
        out_shape=jax.ShapeDtypeStruct((n, group_count, slots, quarter, tile), dtype),
        in_specs=[
            pl.BlockSpec(memory_space=pl.ANY),
            pl.BlockSpec(memory_space=pltpu.VMEM),
        ],
        out_specs=pl.BlockSpec(memory_space=pl.ANY),
        scratch_shapes=[
            pltpu.VMEM(density_tiles.shape, dtype),
            pltpu.VMEM((cells * n + 1, per_layer, slots, tile, tile), dtype),
            pltpu.VMEM((cells * n, 1, lanes), jnp.int32),
            pltpu.SMEM((cells * n, 1, lanes), jnp.int32),
            pltpu.VMEM((layer_count, n, per_layer, slots, quarter, tile), dtype),
            pltpu.SemaphoreType.DMA((4,)),
            pltpu.SemaphoreType.DMA((cells,)),
            pltpu.SemaphoreType.DMA((cells,)),
            pltpu.SemaphoreType.DMA((4, cells, chunks)),
            pltpu.SemaphoreType.DMA((cells, chunks)),
            pltpu.SemaphoreType.DMA,
            pltpu.SemaphoreType.DMA,
            pltpu.SemaphoreType.DMA((layer_count, out_chunks)),
            pltpu.SemaphoreType.DMA((layer_count, out_chunks)),
        ],
        compiler_params=pltpu.CompilerParams(
            collective_id=1, has_side_effects=True, vmem_limit_bytes=60 * 1024 * 1024
        ),
    )(density_tiles, meta)


def solution(mesh):
    paired = mesh.shape["row"] == 2 and mesh.shape["layer"] % 2 == 0
    in_specs = (P(("row", "col"), None, None, None, None), P(("row", "col"), None, None))
    out_specs = P(("row", "col"), None, None, "layer", None)
    return jax.shard_map(
        on_device_paired if paired else on_device, mesh=mesh, in_specs=in_specs, out_specs=out_specs, check_vma=False
    )
```

```python
import functools

import jax
import jax.numpy as jnp
from jax import lax
from jax.experimental import pallas as pl
from jax.experimental.pallas import tpu as pltpu
from jax.sharding import PartitionSpec as P

MESH = pl.DeviceIdType.MESH


def divisor(total, most):
    return max(d for d in range(1, most + 1) if total % d == 0)


def kernel(
    sizes, columns_ref, tiles_ref, meta_ref, out_ref,
    left, right, meta_all, meta_smem, stage,
    local_sem, meta_send, meta_recv, send_sem, recv_sem, out_send, out_recv,
):
    row_count, col_count, layer_count, chunks, out_chunks, is_balanced = sizes
    n, group_count, slots, tile, _ = tiles_ref.shape
    cells = row_count * col_count
    per_layer = group_count // layer_count
    quarter = tile // layer_count
    width = group_count * slots
    r, c, l = lax.axis_index("row"), lax.axis_index("col"), lax.axis_index("layer")
    me = r * col_count + c
    own_groups = pl.ds(l * per_layer, per_layer)

    own_copy = pltpu.make_async_copy(
        tiles_ref.at[:, own_groups], right.at[pl.ds(me * n, n)], local_sem.at[0]
    )
    left_copy = pltpu.make_async_copy(tiles_ref, left, local_sem.at[1])
    meta_copy = pltpu.make_async_copy(meta_ref, meta_all.at[pl.ds(me * n, n)], local_sem.at[2])
    own_copy.start()
    meta_copy.start()
    left_copy.start()
    right[cells * n] = jnp.zeros(right.shape[1:], right.dtype)

    def cell_id(offset):
        target = lax.rem(me + offset, cells)
        return {"row": lax.div(target, col_count), "col": lax.rem(target, col_count)}

    def layer_id(offset):
        return {"layer": lax.rem(l + offset, layer_count)}

    barrier = pltpu.get_barrier_semaphore()
    for offset in range(1, cells):
        pl.semaphore_signal(barrier, inc=1, device_id=cell_id(offset), device_id_type=MESH)
    for offset in range(1, layer_count):
        pl.semaphore_signal(barrier, inc=1, device_id=layer_id(offset), device_id_type=MESH)
    pl.semaphore_wait(barrier, cells - 1 + layer_count - 1)
    own_copy.wait()

    step_rows = n // chunks
    sent = []

    def rows_of(cell, chunk):
        return pl.ds(cell * n + chunk * step_rows, step_rows)

    def copy_of(cell, chunk, way, device):
        return pltpu.make_async_remote_copy(
            src_ref=right.at[rows_of(cell, chunk)],
            dst_ref=right.at[rows_of(cell, chunk)],
            send_sem=send_sem.at[way, cell, chunk],
            recv_sem=recv_sem.at[cell, chunk],
            device_id=device,
            device_id_type=MESH,
        )

    ways = {
        "up": (0, c < col_count - 1, {"col": jnp.minimum(c + 1, col_count - 1)}),
        "down": (1, c > 0, {"col": jnp.maximum(c - 1, 0)}),
        "south": (2, r < row_count - 1, {"row": jnp.minimum(r + 1, row_count - 1)}),
        "north": (3, r > 0, {"row": jnp.maximum(r - 1, 0)}),
    }

    def send(cell, chunk, way, condition=True):
        index, exists, device = ways[way]
        wanted = jnp.logical_and(exists, condition)

        @pl.when(wanted)
        def _():
            copy_of(cell, chunk, index, device).start()

        sent.append((wanted, cell, chunk, index, device))

    def await_arrival(cell, chunk):
        copy_of(cell, chunk, 0, {"col": c}).wait_recv()

    for chunk in range(chunks):
        for way in ("up", "down", "south", "north"):
            send(me, chunk, way)

    meta_copy.wait()
    meta_copies = []
    for offset in range(1, cells):
        copy = pltpu.make_async_remote_copy(
            src_ref=meta_ref,
            dst_ref=meta_all.at[pl.ds(me * n, n)],
            send_sem=meta_send.at[offset],
            recv_sem=meta_recv.at[offset],
            device_id=cell_id(offset),
            device_id_type=MESH,
        )
        copy.start()
        meta_copies.append(copy)

    even = lax.rem(c, 2) == 0
    for step in range(1, col_count):
        for chunk in range(chunks):
            for origin, has, way, is_pair in (
                (c - step, c >= step, "up", jnp.logical_not(even)),
                (c + step, c + step < col_count, "down", even),
            ):
                origin = jnp.clip(origin, 0, col_count - 1)
                cell = r * col_count + origin

                @pl.when(has)
                def _():
                    await_arrival(cell, chunk)

                send(cell, chunk, way, has)
                across = has
                if is_balanced and step == 1 and chunk >= chunks // 2:
                    across = jnp.logical_and(has, jnp.logical_not(is_pair))
                send(cell, chunk, "south", across)
                send(cell, chunk, "north", across)

    if is_balanced:
        other = (1 - r) * col_count + c
        for chunk in range(chunks):
            await_arrival(other, chunk)
            if chunk >= chunks // 2:
                send(other, chunk, "up", even)
                send(other, chunk, "down", jnp.logical_not(even))
        for step in range(1, col_count):
            origin = (1 - r) * col_count + lax.rem(c + step, col_count)
            for chunk in range(chunks):
                await_arrival(origin, chunk)
    else:
        for step in range(1, row_count):
            for shift in range(col_count):
                for chunk in range(chunks):
                    for origin, has, way in (
                        (r - step, r >= step, "south"),
                        (r + step, r + step < row_count, "north"),
                    ):
                        origin = jnp.clip(origin, 0, row_count - 1)
                        cell = origin * col_count + lax.rem(c + shift, col_count)

                        @pl.when(has)
                        def _():
                            await_arrival(cell, chunk)

                        send(cell, chunk, way, has)

    for copy in meta_copies:
        copy.wait()
    table_copy = pltpu.make_async_copy(meta_all, meta_smem, local_sem.at[3])
    table_copy.start()
    table_copy.wait()
    left_copy.wait()

    def one_row(i, carry):
        targets = [
            columns_ref[i * width + l * per_layer * slots + s] for s in range(per_layer * slots)
        ]
        strips = []
        for a in range(width):
            k = columns_ref[i * width + a]
            inner = jnp.maximum(k, 0)
            pieces = []
            for s in range(per_layer * slots):
                group = s // slots
                row_index = jnp.int32(cells * n)
                slot_index = jnp.int32(0)
                is_live = (k >= 0) & (targets[s] >= 0)
                for t in range(slots):
                    hit = (meta_smem[inner, 0, group * slots + t] == targets[s]) & is_live
                    row_index = jnp.where(hit, inner, row_index)
                    slot_index = jnp.where(hit, t, slot_index)
                pieces.append(right[row_index, group, slot_index])
            strips.append(jnp.concatenate(pieces, axis=1))
        rights = jnp.concatenate(strips, axis=0)
        lefts = jnp.concatenate(
            [left[i, a // slots, a % slots] for a in range(width)], axis=1
        )
        total = jnp.dot(lefts, rights, preferred_element_type=jnp.float32).astype(stage.dtype)
        for q in range(layer_count):
            for s in range(per_layer * slots):
                stage[q, i, s // slots, s % slots] = total[
                    q * quarter:(q + 1) * quarter, s * tile:(s + 1) * tile
                ]
        return carry

    out_rows = n // out_chunks

    def out_copies(chunk):
        rows = pl.ds(chunk * out_rows, out_rows)
        copies = []
        for offset in range(layer_count):
            q = lax.rem(l + offset, layer_count)
            if offset == 0:
                copies.append(pltpu.make_async_copy(
                    stage.at[q, rows], out_ref.at[rows, own_groups], out_send.at[0, chunk]
                ))
            else:
                copies.append(pltpu.make_async_remote_copy(
                    src_ref=stage.at[q, rows],
                    dst_ref=out_ref.at[rows, own_groups],
                    send_sem=out_send.at[offset, chunk],
                    recv_sem=out_recv.at[offset, chunk],
                    device_id=layer_id(offset),
                    device_id_type=MESH,
                ))
        return copies

    all_out = []
    for chunk in range(out_chunks + 1):
        if chunk < out_chunks:
            lax.fori_loop(chunk * out_rows, (chunk + 1) * out_rows, one_row, 0)
        if chunk > 0:
            copies = out_copies(chunk - 1)
            for copy in copies[1:] + copies[:1]:
                copy.start()
            all_out.extend(copies)

    for wanted, cell, chunk, index, device in sent:
        @pl.when(wanted)
        def _():
            copy_of(cell, chunk, index, device).wait_send()

    for copy in all_out:
        copy.wait()


def on_device(density_tiles, tile_columns):
    row_count = lax.axis_size("row")
    col_count = lax.axis_size("col")
    layer_count = lax.axis_size("layer")
    n, group_count, slots, tile, _ = density_tiles.shape
    cells = row_count * col_count
    per_layer = group_count // layer_count
    quarter = tile // layer_count
    kept = per_layer * slots
    chunks = divisor(n, 4)
    out_chunks = divisor(n, 4)
    is_balanced = row_count == 2 and col_count % 2 == 0 and chunks % 2 == 0
    own = lax.dynamic_slice_in_dim(tile_columns, lax.axis_index("layer") * per_layer, per_layer, 1)
    meta = jnp.pad(own.reshape(n, 1, kept), ((0, 0), (0, 0), (0, 128 - kept)), constant_values=-1)
    dtype = density_tiles.dtype
    sizes = (row_count, col_count, layer_count, chunks, out_chunks, is_balanced)
    return pl.pallas_call(
        functools.partial(kernel, sizes),
        out_shape=jax.ShapeDtypeStruct((n, group_count, slots, quarter, tile), dtype),
        in_specs=[
            pl.BlockSpec(memory_space=pltpu.SMEM),
            pl.BlockSpec(memory_space=pl.ANY),
            pl.BlockSpec(memory_space=pltpu.VMEM),
        ],
        out_specs=pl.BlockSpec(memory_space=pl.ANY),
        scratch_shapes=[
            pltpu.VMEM(density_tiles.shape, dtype),
            pltpu.VMEM((cells * n + 1, per_layer, slots, tile, tile), dtype),
            pltpu.VMEM((cells * n, 1, 128), jnp.int32),
            pltpu.SMEM((cells * n, 1, 128), jnp.int32),
            pltpu.VMEM((layer_count, n, per_layer, slots, quarter, tile), dtype),
            pltpu.SemaphoreType.DMA((4,)),
            pltpu.SemaphoreType.DMA((cells,)),
            pltpu.SemaphoreType.DMA((cells,)),
            pltpu.SemaphoreType.DMA((4, cells, chunks)),
            pltpu.SemaphoreType.DMA((cells, chunks)),
            pltpu.SemaphoreType.DMA((layer_count, out_chunks)),
            pltpu.SemaphoreType.DMA((layer_count, out_chunks)),
        ],
        compiler_params=pltpu.CompilerParams(
            collective_id=0, has_side_effects=True, vmem_limit_bytes=60 * 1024 * 1024
        ),
    )(tile_columns.reshape(-1), density_tiles, meta)


def paired_kernel(
    sizes, tiles_ref, meta_ref, out_ref,
    left, right, meta_all, meta_smem, stage,
    local_sem, meta_send, meta_recv, send_sem, recv_sem, left_send, left_recv, out_send, out_recv,
):
    col_count, layer_count, chunks, out_chunks = sizes
    n, group_count, slots, tile, _ = tiles_ref.shape
    cells = 2 * col_count
    per_layer = group_count // layer_count
    quarter = tile // layer_count
    width = group_count * slots
    r, c, l = lax.axis_index("row"), lax.axis_index("col"), lax.axis_index("layer")
    high, k = lax.div(l, 2), lax.rem(l, 2)
    me = r * col_count + c
    base = k * col_count + c
    is_home = k == r
    is_guest = jnp.logical_not(is_home)
    group = 2 * high + r
    own_groups = pl.ds(group * per_layer, per_layer)
    other_groups = pl.ds((2 * high + 1 - r) * per_layer, per_layer)
    facing = {"row": 1 - r}
    partner = {"layer": 2 * high + 1 - k}

    own_copy = pltpu.make_async_copy(
        tiles_ref.at[:, own_groups], right.at[pl.ds(me * n, n)], local_sem.at[0]
    )
    left_copy = pltpu.make_async_copy(tiles_ref, left, local_sem.at[1])
    meta_copy = pltpu.make_async_copy(meta_ref, meta_all.at[pl.ds(me * n, n)], local_sem.at[2])
    own_copy.start()
    meta_copy.start()

    @pl.when(is_home)
    def _():
        left_copy.start()

    right[cells * n] = jnp.zeros(right.shape[1:], right.dtype)

    def cell_id(offset):
        target = lax.rem(me + offset, cells)
        return {"row": lax.div(target, col_count), "col": lax.rem(target, col_count)}

    barrier = pltpu.get_barrier_semaphore()
    for offset in range(1, cells):
        pl.semaphore_signal(barrier, inc=1, device_id=cell_id(offset), device_id_type=MESH)
    for offset in range(1, layer_count):
        for row in (r, 1 - r):
            pl.semaphore_signal(
                barrier,
                inc=1,
                device_id={"row": row, "layer": lax.rem(l + offset, layer_count)},
                device_id_type=MESH,
            )
    pl.semaphore_wait(barrier, cells - 1 + 2 * (layer_count - 1))

    step_rows = n // chunks
    sent = []

    def rows_of(cell, chunk):
        return pl.ds(cell * n + chunk * step_rows, step_rows)

    def copy_of(cell, chunk, way, device):
        source = right.at[rows_of(cell, chunk)]
        if way == 3:
            source = tiles_ref.at[pl.ds(chunk * step_rows, step_rows), other_groups]
        return pltpu.make_async_remote_copy(
            src_ref=source,
            dst_ref=right.at[rows_of(cell, chunk)],
            send_sem=send_sem.at[way, cell, chunk],
            recv_sem=recv_sem.at[cell, chunk],
            device_id=device,
            device_id_type=MESH,
        )

    ways = {
        "up": (0, c < col_count - 1, {"col": jnp.minimum(c + 1, col_count - 1)}),
        "down": (1, c > 0, {"col": jnp.maximum(c - 1, 0)}),
        "partner": (2, True, partner),
        "facing": (3, True, facing),
    }

    def send(cell, chunk, way, condition):
        index, exists, device = ways[way]
        wanted = jnp.logical_and(exists, condition)

        @pl.when(wanted)
        def _():
            copy_of(cell, chunk, index, device).start()

        sent.append((wanted, cell, chunk, index, device))

    def await_arrival(cell, chunk, condition):
        @pl.when(condition)
        def _():
            copy_of(cell, chunk, 2, partner).wait_recv()

    for chunk in range(chunks):
        send(me, chunk, "facing", is_home)
    own_copy.wait()
    for chunk in range(chunks):
        for way in ("up", "down"):
            send(me, chunk, way, is_home)
    left_out = pltpu.make_async_remote_copy(
        src_ref=tiles_ref, dst_ref=left, send_sem=left_send, recv_sem=left_recv,
        device_id=facing, device_id_type=MESH,
    )

    meta_copy.wait()
    meta_copies = []
    for offset in range(1, cells):
        copy = pltpu.make_async_remote_copy(
            src_ref=meta_ref,
            dst_ref=meta_all.at[pl.ds(me * n, n)],
            send_sem=meta_send.at[offset],
            recv_sem=meta_recv.at[offset],
            device_id=cell_id(offset),
            device_id_type=MESH,
        )
        copy.start()
        meta_copies.append(copy)

    @pl.when(is_home)
    def _():
        left_out.start()

    for chunk in range(chunks):
        await_arrival(base, chunk, is_guest)
        for way in ("up", "down", "partner"):
            send(base, chunk, way, is_guest)

    for step in range(1, col_count):
        for chunk in range(chunks):
            for origin, has, way in (
                (c - step, c >= step, "up"),
                (c + step, c + step < col_count, "down"),
            ):
                cell = k * col_count + jnp.clip(origin, 0, col_count - 1)
                await_arrival(cell, chunk, has)
                send(cell, chunk, way, has)
                send(cell, chunk, "partner", has)

    for chunk in range(chunks):
        await_arrival((1 - k) * col_count + c, chunk, is_home)
    for step in range(1, col_count):
        cell = (1 - k) * col_count + lax.rem(c + step, col_count)
        for chunk in range(chunks):
            await_arrival(cell, chunk, True)

    for copy in meta_copies:
        copy.wait()
    table_copy = pltpu.make_async_copy(meta_all, meta_smem, local_sem.at[3])
    table_copy.start()
    table_copy.wait()

    @pl.when(is_home)
    def _():
        left_copy.wait()

    @pl.when(is_guest)
    def _():
        left_out.wait_recv()

    first = group * per_layer * slots

    def one_row(i, carry):
        block_row = base * n + i
        targets = [meta_smem[block_row, 0, first + s] for s in range(per_layer * slots)]
        strips = []
        for a in range(width):
            column = meta_smem[block_row, 0, a]
            inner = jnp.maximum(column, 0)
            pieces = []
            for s in range(per_layer * slots):
                part = s // slots
                row_index = jnp.int32(cells * n)
                slot_index = jnp.int32(0)
                is_live = (column >= 0) & (targets[s] >= 0)
                for t in range(slots):
                    hit = (meta_smem[inner, 0, first + part * slots + t] == targets[s]) & is_live
                    row_index = jnp.where(hit, inner, row_index)
                    slot_index = jnp.where(hit, t, slot_index)
                pieces.append(right[row_index, part, slot_index])
            strips.append(jnp.concatenate(pieces, axis=1))
        rights = jnp.concatenate(strips, axis=0)
        lefts = jnp.concatenate(
            [left[i, a // slots, a % slots] for a in range(width)], axis=1
        )
        total = jnp.dot(lefts, rights, preferred_element_type=jnp.float32).astype(stage.dtype)
        for q in range(layer_count):
            for s in range(per_layer * slots):
                stage[q, i, s // slots, s % slots] = total[
                    q * quarter:(q + 1) * quarter, s * tile:(s + 1) * tile
                ]
        return carry

    out_rows = n // out_chunks

    def out_copy(chunk, q, source):
        rows = pl.ds(chunk * out_rows, out_rows)
        return pltpu.make_async_remote_copy(
            src_ref=stage.at[q, rows],
            dst_ref=out_ref.at[rows, pl.ds(source * per_layer, per_layer)],
            send_sem=out_send.at[q, chunk],
            recv_sem=out_recv.at[source, chunk],
            device_id={"row": k, "layer": q},
            device_id_type=MESH,
        )

    def kept_copy(chunk):
        rows = pl.ds(chunk * out_rows, out_rows)
        return pltpu.make_async_copy(
            stage.at[l, rows], out_ref.at[rows, own_groups], out_send.at[l, chunk]
        )

    for chunk in range(out_chunks + 1):
        if chunk < out_chunks:
            lax.fori_loop(chunk * out_rows, (chunk + 1) * out_rows, one_row, 0)
        if chunk > 0:
            for offset in range(layer_count - 1, -1, -1):
                q = lax.rem(l + offset, layer_count)
                if offset:
                    out_copy(chunk - 1, q, group).start()
                else:
                    @pl.when(is_guest)
                    def _():
                        out_copy(chunk - 1, q, group).start()

                    @pl.when(is_home)
                    def _():
                        kept_copy(chunk - 1).start()

    for wanted, cell, chunk, index, device in sent:
        @pl.when(wanted)
        def _():
            copy_of(cell, chunk, index, device).wait_send()

    @pl.when(is_home)
    def _():
        left_out.wait_send()

    for chunk in range(out_chunks):
        for offset in range(layer_count):
            q = lax.rem(l + offset, layer_count)
            source = lax.rem(group + offset, layer_count)
            if offset:
                out_copy(chunk, q, source).wait()
            else:
                @pl.when(is_guest)
                def _():
                    out_copy(chunk, q, source).wait()

                @pl.when(is_home)
                def _():
                    kept_copy(chunk).wait()


def on_device_paired(density_tiles, tile_columns):
    col_count = lax.axis_size("col")
    layer_count = lax.axis_size("layer")
    n, group_count, slots, tile, _ = density_tiles.shape
    cells = 2 * col_count
    per_layer = group_count // layer_count
    quarter = tile // layer_count
    width = group_count * slots
    chunks = divisor(n, 2)
    out_chunks = divisor(n, 12)
    lanes = -(-width // 128) * 128
    meta = jnp.pad(
        tile_columns.reshape(n, 1, width), ((0, 0), (0, 0), (0, lanes - width)), constant_values=-1
    )
    dtype = density_tiles.dtype
    return pl.pallas_call(
        functools.partial(paired_kernel, (col_count, layer_count, chunks, out_chunks)),
        out_shape=jax.ShapeDtypeStruct((n, group_count, slots, quarter, tile), dtype),
        in_specs=[
            pl.BlockSpec(memory_space=pl.ANY),
            pl.BlockSpec(memory_space=pltpu.VMEM),
        ],
        out_specs=pl.BlockSpec(memory_space=pl.ANY),
        scratch_shapes=[
            pltpu.VMEM(density_tiles.shape, dtype),
            pltpu.VMEM((cells * n + 1, per_layer, slots, tile, tile), dtype),
            pltpu.VMEM((cells * n, 1, lanes), jnp.int32),
            pltpu.SMEM((cells * n, 1, lanes), jnp.int32),
            pltpu.VMEM((layer_count, n, per_layer, slots, quarter, tile), dtype),
            pltpu.SemaphoreType.DMA((4,)),
            pltpu.SemaphoreType.DMA((cells,)),
            pltpu.SemaphoreType.DMA((cells,)),
            pltpu.SemaphoreType.DMA((4, cells, chunks)),
            pltpu.SemaphoreType.DMA((cells, chunks)),
            pltpu.SemaphoreType.DMA,
            pltpu.SemaphoreType.DMA,
            pltpu.SemaphoreType.DMA((layer_count, out_chunks)),
            pltpu.SemaphoreType.DMA((layer_count, out_chunks)),
        ],
        compiler_params=pltpu.CompilerParams(
            collective_id=1, has_side_effects=True, vmem_limit_bytes=60 * 1024 * 1024
        ),
    )(density_tiles, meta)


def solution(mesh):
    paired = mesh.shape["row"] == 2 and mesh.shape["layer"] % 2 == 0
    in_specs = (P(("row", "col"), None, None, None, None), P(("row", "col"), None, None))
    out_specs = P(("row", "col"), None, None, "layer", None)
    return jax.shard_map(
        on_device_paired if paired else on_device, mesh=mesh, in_specs=in_specs, out_specs=out_specs, check_vma=False
    )
```
